32 devices in a mesh: site: 2 (over y), rows: 4 (over z), cols: 2 (over core), slabs: 2 (over x).
Axes of the slice: x: 2, y: 2, z: 4, core: 2. Of those that a mesh axis runs over, the one named last changes fastest.
Arguments:
- pressure: float32 [32, 128, 64, 128], P(('site', 'rows'), 'cols', 'slabs'), parts along dimension 0, may hold values from 0.2 to 1.8
- earlier: float32 [32, 128, 64, 128], P(('site', 'rows'), 'cols', 'slabs'), parts along dimension 0, may hold values from 0.2 to 1.8
- speed_square: float32 [32, 128, 64, 128], P(('site', 'rows'), 'cols', 'slabs'), parts along dimension 0, may hold values from 0.05 to 0.3
Outputs:
- potential: float32 [32, 128, 64, 128], P(('site', 'rows'), 'cols', 'slabs'), parts along dimension 0
- pressure_end: float32 [32, 128, 64, 128], P(('site', 'rows'), 'cols', 'slabs'), parts along dimension 0
The draws below stay inside these ranges and needn't reach their ends.
There are 2 independent parts, one for each index of `site`. The reference program is written for one: setup_inputs(seed, part) draws one part's arguments, and reference() takes and returns one part's arrays. A program takes and returns all parts, laid end to end along the dimension named above; each array names one. Nothing has to cross between parts.
All inputs are finite; a program needn't handle non-finite values.
Results may differ from the reference program's by a relative error of at most 0.00002.
Values sent between devices are 32-bit elements; how exact they have to be, the bound alone decides.
A program may use at most 192 MiB of HBM per device.

```python
import jax
import jax.numpy as jnp
from jax import lax

GRID_J = 16
GRID_I = 128
GRID_K = 64
MEMBERS = 128
STEPS = 4


def steps_of(rng, extent, split, low, high):
    def one(dim, shards_of):
        draws = jax.random.uniform(jax.random.fold_in(jax.random.fold_in(rng, 6), dim), (shards_of,), jnp.float32, low / len(split), high / len(split))
        return jnp.repeat(jnp.exp(draws), extent[dim] // shards_of).reshape((-1,) + (1,) * (len(extent) - dim - 1))

    gain = one(*split[0])
    for cut in split[1:]:
        gain = gain * one(*cut)
    return gain


def setup_inputs(seed: int = 0, part: int = 0) -> dict:
    key_list = jax.random.split(jax.random.key(seed), 4)
    part_keys = jax.random.split(jax.random.fold_in(key_list[3], part), 4)
    return {
        "pressure": jnp.clip(0.2 + 1.5999999 * jax.random.uniform(part_keys[0], (GRID_J, GRID_I, GRID_K, MEMBERS), jnp.float32) ** steps_of(part_keys[0], (GRID_J, GRID_I, GRID_K, MEMBERS), ((0, 4), (1, 2), (2, 2)), -0.2, 0.2), 0.2, 1.8),
        "earlier": jnp.clip(0.2 + 1.5999999 * jax.random.uniform(part_keys[1], (GRID_J, GRID_I, GRID_K, MEMBERS), jnp.float32) ** steps_of(part_keys[1], (GRID_J, GRID_I, GRID_K, MEMBERS), ((0, 4), (1, 2), (2, 2)), -0.2, 0.2), 0.2, 1.8),
        "speed_square": jnp.clip(0.05 + 0.25 * jax.random.uniform(part_keys[2], (GRID_J, GRID_I, GRID_K, MEMBERS), jnp.float32) ** steps_of(part_keys[2], (GRID_J, GRID_I, GRID_K, MEMBERS), ((0, 4), (1, 2), (2, 2)), -0.2, 0.2), 0.05, 0.3),
    }


def strip_edges(values, dims):
    for dim in dims:
        values = lax.slice_in_dim(values, 1, values.shape[dim] - 1, axis=dim)
    return values


def neighbour(values, dim, start, dims):
    others = [other for other in dims if other != dim]
    values = strip_edges(values, others)
    return lax.slice_in_dim(values, start, start + values.shape[dim] - 2, axis=dim)


def one_step(padded, before, speed_square):
    middle = strip_edges(padded, (0, 1, 2))
    lower = [neighbour(padded, dim, 0, (0, 1, 2)) for dim in (0, 1, 2)]
    upper = [neighbour(padded, dim, 2, (0, 1, 2)) for dim in (0, 1, 2)]
    spread = lower[0] + upper[0] + lower[1] + upper[1] + lower[2] + upper[2] - 6.0 * middle
    return 2.0 * middle - before + speed_square * spread


def reference(pressure, earlier, speed_square):
    for step in range(STEPS):
        later = one_step(jnp.pad(pressure, ((1, 1), (1, 1), (1, 1), (0, 0)), mode="wrap"), earlier, speed_square)
        earlier, pressure = pressure, later
    potential = jnp.cumsum(pressure, axis=0) / GRID_J
    return potential, pressure
```

```python
import functools

import jax
import jax.numpy as jnp
from jax import lax
from jax.experimental import pallas as pl
from jax.experimental.pallas import tpu as pltpu
from jax.sharding import PartitionSpec as P

STEPS = 4
MESH = pl.DeviceIdType.MESH
RING_AXES = ("rows", "cols", "slabs")


def kernel(
    ring, parts, total,
    p_in, e_in, c_in, pot_out, end_out,
    field, speed, side_out, side_in, below, sums,
    load_sem, z_send, z_recv, k_send, k_recv, i_send, i_recv, t_send, t_recv, out_sem,
):
    nj, ni, nk, _ = p_in.shape
    width = ni // parts
    row = lax.axis_index("rows")
    places = {axis: lax.axis_index(axis) for axis in RING_AXES}
    after = {axis: {axis: lax.rem(places[axis] + 1, ring[axis])} for axis in RING_AXES}
    before = {
        axis: {axis: lax.rem(places[axis] + ring[axis] - 1, ring[axis])} for axis in RING_AXES
    }

    def piece_of(q):
        half = q // 2
        return jnp.where(q % 2 == 0, half, parts - 1 - half)

    def rim(c):
        return pl.ds(1 + c * width, width)

    def inner(c):
        return pl.ds(c * width, width)

    def load(which, c):
        src = (p_in, e_in, c_in)[which].at[:, inner(c)]
        if which == 2:
            dst = speed.at[:, inner(c)]
        else:
            dst = field.at[1 - which, pl.ds(1, nj), rim(c)]
        return pltpu.make_async_copy(src, dst, load_sem.at[which, c])

    def remote(src, dst, send, recv, where):
        return pltpu.make_async_remote_copy(
            src_ref=src, dst_ref=dst, send_sem=send, recv_sem=recv,
            device_id=where, device_id_type=MESH,
        )

    def z_copy(t, way, c):
        src = field.at[t + 1, nj if way == 0 else 1, rim(c)]
        dst = field.at[t + 1, 0 if way == 0 else nj + 1, rim(c)]
        where = after["rows"] if way == 0 else before["rows"]
        return remote(src, dst, z_send.at[t, way, c], z_recv.at[t, way, c], where)

    def k_copy(t, way, c):
        where = after["slabs"] if way == 0 else before["slabs"]
        return remote(
            side_out.at[t, way, :, inner(c)], side_in.at[t, way, :, inner(c)],
            k_send.at[t, way, c], k_recv.at[t, way, c], where,
        )

    def i_copy(t, way):
        src = field.at[t + 1, pl.ds(1, nj), ni if way == 0 else 1]
        dst = field.at[t + 1, pl.ds(1, nj), 0 if way == 0 else ni + 1]
        where = after["cols"] if way == 0 else before["cols"]
        return remote(src, dst, i_send.at[t, way], i_recv.at[t, way], where)

    def t_copy(c):
        return remote(
            sums.at[inner(c)], below.at[inner(c)], t_send.at[c], t_recv.at[c], after["rows"]
        )

    def out_copy(which, c):
        src = field.at[STEPS + 1 if which == 0 else 0, pl.ds(1, nj), rim(c)]
        dst = (end_out, pot_out)[which].at[:, inner(c)]
        return pltpu.make_async_copy(src, dst, out_sem.at[which, c])

    def send_all(t, c):
        z_copy(t, 0, c).start()
        z_copy(t, 1, c).start()
        k_copy(t, 0, c).start()
        k_copy(t, 1, c).start()

        @pl.when(c == parts - 1)
        def _():
            i_copy(t, 0).start()

        @pl.when(c == 0)
        def _():
            i_copy(t, 1).start()

    def each(count, body):
        def wrapped(n, carry):
            body(n)
            return carry

        lax.fori_loop(0, count, wrapped, 0)

    for which in range(3):
        each(parts, lambda q: load(which, piece_of(q)).start())

    barrier = pltpu.get_barrier_semaphore()
    for axis in RING_AXES:
        for where in (after[axis], before[axis]):
            pl.semaphore_signal(barrier, inc=1, device_id=where, device_id_type=MESH)
    pl.semaphore_wait(barrier, 2 * len(RING_AXES))

    def begin(q):
        c = piece_of(q)
        load(0, c).wait()

        def sides(n):
            i = c * width + n
            for j in range(nj):
                side_out[0, 0, j, i] = field[1, j + 1, i + 1, nk - 1:nk]
                side_out[0, 1, j, i] = field[1, j + 1, i + 1, 0:1]

        each(width, sides)
        send_all(0, c)

    each(parts, begin)

    def wait_loads(q):
        load(1, piece_of(q)).wait()
        load(2, piece_of(q)).wait()

    each(parts, wait_loads)

    def advance(t, q, last):
        c = piece_of(q)
        k_copy(t, 0, c).wait_recv()
        k_copy(t, 1, c).wait_recv()

        @pl.when(c == 0)
        def _():
            i_copy(t, 0).wait_recv()

        @pl.when(c == parts - 1)
        def _():
            i_copy(t, 1).wait_recv()

        z_copy(t, 0, c).wait_recv()
        z_copy(t, 1, c).wait_recv()

        def line(n):
            i = c * width + n
            level = lax.broadcasted_iota(jnp.int32, (nk, 1), 0)
            column = [field[t + 1, j, i + 1] for j in range(nj + 2)]
            run = None
            for j in range(nj):
                middle = column[j + 1]
                under = jnp.where(level == 0, side_in[t, 0, j, i], pltpu.roll(middle, 1, 0))
                over = jnp.where(
                    level == nk - 1, side_in[t, 1, j, i], pltpu.roll(middle, nk - 1, 0)
                )
                spread = (
                    column[j] + column[j + 2] + field[t + 1, j + 1, i] + field[t + 1, j + 1, i + 2]
                    + under + over - 6.0 * middle
                )
                later = 2.0 * middle - field[t, j + 1, i + 1] + speed[j, i] * spread
                field[t + 2, j + 1, i + 1] = later
                if last:
                    run = later if run is None else run + later
                    field[0, j + 1, i + 1] = run
                else:
                    side_out[t + 1, 0, j, i] = later[nk - 1:nk]
                    side_out[t + 1, 1, j, i] = later[0:1]
            if last:
                sums[i] = run

        each(width, line)
        if last:
            @pl.when(row == 0)
            def _():
                t_copy(c).start()

            out_copy(0, c).start()
        else:
            send_all(t + 1, c)

    each(STEPS - 1, lambda t: each(parts, lambda q: advance(t, q, False)))
    each(parts, lambda q: advance(STEPS - 1, q, True))

    def finish(q):
        c = piece_of(q)

        @pl.when(row > 0)
        def _():
            t_copy(c).wait_recv()

            @pl.when(row < ring["rows"] - 1)
            def _():
                def passed(n):
                    i = c * width + n
                    sums[i] = sums[i] + below[i]

                each(width, passed)
                t_copy(c).start()

            def added(n):
                i = c * width + n
                base = below[i]
                for j in range(nj):
                    field[0, j + 1, i + 1] = (field[0, j + 1, i + 1] + base) / total

            each(width, added)

        @pl.when(row == 0)
        def _():
            def scaled(n):
                i = c * width + n
                for j in range(nj):
                    field[0, j + 1, i + 1] = field[0, j + 1, i + 1] / total

            each(width, scaled)

        out_copy(1, c).start()

    each(parts, finish)

    def drain(c):
        def steps(t):
            for way in range(2):
                z_copy(t, way, c).wait_send()
                k_copy(t, way, c).wait_send()

        each(STEPS, steps)

        @pl.when(row < ring["rows"] - 1)
        def _():
            t_copy(c).wait_send()

        out_copy(0, c).wait()
        out_copy(1, c).wait()

    each(parts, drain)

    def drain_ends(t):
        i_copy(t, 0).wait_send()
        i_copy(t, 1).wait_send()

    each(STEPS, drain_ends)


def local(pressure, earlier, speed_square):
    nj, ni, nk, nm = pressure.shape
    ring = {axis: lax.axis_size(axis) for axis in RING_AXES}
    parts = 8 if ni % 8 == 0 else 2
    total = float(nj * ring["rows"])
    anywhere = pl.BlockSpec(memory_space=pl.ANY)
    shape = jax.ShapeDtypeStruct(pressure.shape, jnp.float32)
    dma = pltpu.SemaphoreType.DMA
    return pl.pallas_call(
        functools.partial(kernel, ring, parts, total),
        out_shape=(shape, shape),
        in_specs=[anywhere] * 3,
        out_specs=(anywhere, anywhere),
        scratch_shapes=[
            pltpu.VMEM((STEPS + 2, nj + 2, ni + 2, nk, nm), jnp.float32),
            pltpu.VMEM((nj, ni, nk, nm), jnp.float32),
            pltpu.VMEM((STEPS, 2, nj, ni, 1, nm), jnp.float32),
            pltpu.VMEM((STEPS, 2, nj, ni, 1, nm), jnp.float32),
            pltpu.VMEM((ni, nk, nm), jnp.float32),
            pltpu.VMEM((ni, nk, nm), jnp.float32),
            dma((3, parts)),
            dma((STEPS, 2, parts)), dma((STEPS, 2, parts)),
            dma((STEPS, 2, parts)), dma((STEPS, 2, parts)),
            dma((STEPS, 2)), dma((STEPS, 2)),
            dma((parts,)), dma((parts,)),
            dma((2, parts)),
        ],
        compiler_params=pltpu.CompilerParams(
            collective_id=0, has_side_effects=True, vmem_limit_bytes=60 * 1024 * 1024
        ),
    )(pressure, earlier, speed_square)


def solution(mesh):
    placed = P(("site", "rows"), "cols", "slabs", None)
    return jax.shard_map(
        local, mesh=mesh, in_specs=(placed,) * 3, out_specs=(placed,) * 2, check_vma=False
    )
```

```python
import functools

import jax
import jax.numpy as jnp
from jax import lax
from jax.experimental import pallas as pl
from jax.experimental.pallas import tpu as pltpu
from jax.sharding import PartitionSpec as P

STEPS = 4
MESH = pl.DeviceIdType.MESH
RING_AXES = ("rows", "cols", "slabs")


def kernel(
    ring, parts, fine, scale,
    p_in, e_in, c_in, pot_out, end_out,
    field, speed, side_out, side_in, below, sums,
    load_sem, z_send, z_recv, k_send, k_recv, i_send, i_recv, t_send, t_recv,
):
    nj, ni, nk, _ = p_in.shape
    width = ni // parts
    small = ni // fine
    share = fine // parts
    row = lax.axis_index("rows")
    places = {axis: lax.axis_index(axis) for axis in RING_AXES}
    after = {axis: {axis: lax.rem(places[axis] + 1, ring[axis])} for axis in RING_AXES}
    before = {
        axis: {axis: lax.rem(places[axis] + ring[axis] - 1, ring[axis])} for axis in RING_AXES
    }

    def piece_of(q):
        half = q // 2
        return jnp.where(q % 2 == 0, half, parts - 1 - half)

    def rim(c):
        return pl.ds(1 + c * width, width)

    def inner(c):
        return pl.ds(c * width, width)

    def load(which, c):
        src = (p_in, e_in, c_in)[which].at[:, inner(c)]
        if which == 2:
            dst = speed.at[:, inner(c)]
        else:
            dst = field.at[1 - which, pl.ds(1, nj), rim(c)]
        return pltpu.make_async_copy(src, dst, load_sem.at[which, c])

    def remote(src, dst, send, recv, where):
        return pltpu.make_async_remote_copy(
            src_ref=src, dst_ref=dst, send_sem=send, recv_sem=recv,
            device_id=where, device_id_type=MESH,
        )

    def z_copy(t, way, c):
        src = field.at[t + 1, nj if way == 0 else 1, rim(c)]
        dst = field.at[t + 1, 0 if way == 0 else nj + 1, rim(c)]
        where = after["rows"] if way == 0 else before["rows"]
        return remote(src, dst, z_send.at[t, way, c], z_recv.at[t, way, c], where)

    def k_copy(t, way, c):
        where = after["slabs"] if way == 0 else before["slabs"]
        return remote(
            side_out.at[t, way, :, inner(c)], side_in.at[t, way, :, inner(c)],
            k_send.at[t, way, c], k_recv.at[t, way, c], where,
        )

    def i_copy(t, way):
        src = field.at[t + 1, pl.ds(1, nj), ni if way == 0 else 1]
        dst = field.at[t + 1, pl.ds(1, nj), 0 if way == 0 else ni + 1]
        where = after["cols"] if way == 0 else before["cols"]
        return remote(src, dst, i_send.at[t, way], i_recv.at[t, way], where)

    def first_copy(way, c):
        src = p_in.at[nj - 1 if way == 0 else 0, inner(c)]
        dst = field.at[1, 0 if way == 0 else nj + 1, rim(c)]
        where = after["rows"] if way == 0 else before["rows"]
        return remote(src, dst, z_send.at[0, way, c], z_recv.at[0, way, c], where)

    def t_copy(f):
        lines = pl.ds(f * small, small)
        return remote(
            sums.at[lines], below.at[lines], t_send.at[f], t_recv.at[f], after["rows"]
        )

    def send_z(t, c):
        z_copy(t, 0, c).start()
        z_copy(t, 1, c).start()

    def send_sides(t, c):
        k_copy(t, 0, c).start()
        k_copy(t, 1, c).start()

        @pl.when(c == parts - 1)
        def _():
            i_copy(t, 0).start()

        @pl.when(c == 0)
        def _():
            i_copy(t, 1).start()

    def each(count, body):
        def wrapped(n, carry):
            body(n)
            return carry

        lax.fori_loop(0, count, wrapped, 0)

    for which in range(3):
        each(parts, lambda q: load(which, piece_of(q)).start())

    barrier = pltpu.get_barrier_semaphore()
    for axis in RING_AXES:
        for where in (after[axis], before[axis]):
            pl.semaphore_signal(barrier, inc=1, device_id=where, device_id_type=MESH)
    pl.semaphore_wait(barrier, 2 * len(RING_AXES))

    def begin_z(q):
        first_copy(0, piece_of(q)).start()
        first_copy(1, piece_of(q)).start()

    each(parts, begin_z)

    def begin(q):
        c = piece_of(q)
        load(0, c).wait()

        def sides(n):
            i = c * width + n
            for j in range(nj):
                side_out[0, 0, j, i] = field[1, j + 1, i + 1, nk - 1:nk]
                side_out[0, 1, j, i] = field[1, j + 1, i + 1, 0:1]

        each(width, sides)
        send_sides(0, c)

    each(parts, begin)

    def wait_loads(q):
        load(1, piece_of(q)).wait()
        load(2, piece_of(q)).wait()

    each(parts, wait_loads)

    def advance(t, q, last):
        c = piece_of(q)
        k_copy(t, 0, c).wait_recv()
        k_copy(t, 1, c).wait_recv()

        @pl.when(c == 0)
        def _():
            i_copy(t, 0).wait_recv()

        @pl.when(c == parts - 1)
        def _():
            i_copy(t, 1).wait_recv()

        z_copy(t, 0, c).wait_recv()
        z_copy(t, 1, c).wait_recv()

        def line(n):
            i = c * width + n
            level = lax.broadcasted_iota(jnp.int32, (nk, 1), 0)
            column = [field[t + 1, j, i + 1] for j in range(nj + 2)]
            run = None
            for j in range(nj):
                middle = column[j + 1]
                under = jnp.where(level == 0, side_in[t, 0, j, i], pltpu.roll(middle, 1, 0))
                over = jnp.where(
                    level == nk - 1, side_in[t, 1, j, i], pltpu.roll(middle, nk - 1, 0)
                )
                spread = (
                    column[j] + column[j + 2] + field[t + 1, j + 1, i] + field[t + 1, j + 1, i + 2]
                    + under + over - 6.0 * middle
                )
                later = 2.0 * middle - field[t, j + 1, i + 1] + speed[j, i] * spread
                if last:
                    end_out[j, i] = later
                    run = later if run is None else run + later
                    pot_out[j, i] = run
                else:
                    field[t + 2, j + 1, i + 1] = later
                    side_out[t + 1, 0, j, i] = later[nk - 1:nk]
                    side_out[t + 1, 1, j, i] = later[0:1]
            if last:
                sums[i] = run

        each(width, line)
        if last:
            @pl.when(row == 0)
            def _():
                each(share, lambda n: t_copy(c * share + n).start())
        else:
            send_z(t + 1, c)
            send_sides(t + 1, c)

    each(STEPS - 1, lambda t: each(parts, lambda q: advance(t, q, False)))
    each(parts, lambda q: advance(STEPS - 1, q, True))

    def finish(q):
        c = piece_of(q)

        @pl.when(row > 0)
        def _():
            def one(n):
                f = c * share + n
                t_copy(f).wait_recv()

                @pl.when(row < ring["rows"] - 1)
                def _():
                    for m in range(small):
                        sums[f * small + m] = sums[f * small + m] + below[f * small + m]
                    t_copy(f).start()

                for m in range(small):
                    base = below[f * small + m]
                    for j in range(nj):
                        pot_out[j, f * small + m] = scale(pot_out[j, f * small + m] + base)

            each(share, one)

        @pl.when(row == 0)
        def _():
            def scaled(n):
                i = c * width + n
                for j in range(nj):
                    pot_out[j, i] = scale(pot_out[j, i])

            each(width, scaled)

    each(parts, finish)

    def drain(c):
        def steps(t):
            for way in range(2):
                z_copy(t, way, c).wait_send()
                k_copy(t, way, c).wait_send()

        each(STEPS, steps)

        @pl.when(row < ring["rows"] - 1)
        def _():
            each(share, lambda n: t_copy(c * share + n).wait_send())

    each(parts, drain)

    def drain_ends(t):
        i_copy(t, 0).wait_send()
        i_copy(t, 1).wait_send()

    each(STEPS, drain_ends)


def local(pressure, earlier, speed_square):
    nj, ni, nk, nm = pressure.shape
    ring = {axis: lax.axis_size(axis) for axis in RING_AXES}
    parts = 8 if ni % 8 == 0 else 2
    fine = parts * 4 if ni % (parts * 4) == 0 else parts
    cells = nj * ring["rows"]

    def scale(values):
        return values * (1.0 / cells) if cells & (cells - 1) == 0 else values / cells

    anywhere = pl.BlockSpec(memory_space=pl.ANY)
    shape = pltpu.VMEM(pressure.shape, jnp.float32)
    dma = pltpu.SemaphoreType.DMA
    return pl.pallas_call(
        functools.partial(kernel, ring, parts, fine, scale),
        out_shape=(shape, shape),
        in_specs=[anywhere] * 3,
        out_specs=(pl.BlockSpec(memory_space=pltpu.VMEM),) * 2,
        scratch_shapes=[
            pltpu.VMEM((STEPS + 1, nj + 2, ni + 2, nk, nm), jnp.float32),
            pltpu.VMEM((nj, ni, nk, nm), jnp.float32),
            pltpu.VMEM((STEPS, 2, nj, ni, 1, nm), jnp.float32),
            pltpu.VMEM((STEPS, 2, nj, ni, 1, nm), jnp.float32),
            pltpu.VMEM((ni, nk, nm), jnp.float32),
            pltpu.VMEM((ni, nk, nm), jnp.float32),
            dma((3, parts)),
            dma((STEPS, 2, parts)), dma((STEPS, 2, parts)),
            dma((STEPS, 2, parts)), dma((STEPS, 2, parts)),
            dma((STEPS, 2)), dma((STEPS, 2)),
            dma((fine,)), dma((fine,)),
        ],
        compiler_params=pltpu.CompilerParams(
            collective_id=0, has_side_effects=True, vmem_limit_bytes=46 * 1024 * 1024
        ),
    )(pressure, earlier, speed_square)


def solution(mesh):
    placed = P(("site", "rows"), "cols", "slabs", None)
    return jax.shard_map(
        local, mesh=mesh, in_specs=(placed,) * 3, out_specs=(placed,) * 2, check_vma=False
    )
```

```python
import functools

import jax
import jax.numpy as jnp
from jax import lax
from jax.experimental import pallas as pl
from jax.experimental.pallas import tpu as pltpu
from jax.sharding import PartitionSpec as P

STEPS = 4
MESH = pl.DeviceIdType.MESH
RING_AXES = ("rows", "cols", "slabs")


def kernel(
    ring, parts, small, scale,
    p_in, e_in, c_in, pot_out, end_out,
    field, speed, side_out, side_in, below, sums,
    load_sem, z_send, z_recv, k_send, k_recv, i_send, i_recv, t_send, t_recv,
):
    nj, ni, nk, _ = p_in.shape
    width = ni // parts
    row = lax.axis_index("rows")
    places = {axis: lax.axis_index(axis) for axis in RING_AXES}
    after = {axis: {axis: lax.rem(places[axis] + 1, ring[axis])} for axis in RING_AXES}
    before = {
        axis: {axis: lax.rem(places[axis] + ring[axis] - 1, ring[axis])} for axis in RING_AXES
    }

    def piece_of(q):
        half = q // 2
        return jnp.where(q % 2 == 0, half, parts - 1 - half)

    def rim(c):
        return pl.ds(1 + c * width, width)

    def inner(c):
        return pl.ds(c * width, width)

    def load(which, c):
        src = (p_in, e_in, c_in)[which].at[:, inner(c)]
        if which == 2:
            dst = speed.at[:, inner(c)]
        else:
            dst = field.at[1 - which, pl.ds(1, nj), rim(c)]
        return pltpu.make_async_copy(src, dst, load_sem.at[which, c])

    def remote(src, dst, send, recv, where):
        return pltpu.make_async_remote_copy(
            src_ref=src, dst_ref=dst, send_sem=send, recv_sem=recv,
            device_id=where, device_id_type=MESH,
        )

    def z_copy(t, way, c):
        src = field.at[t + 1, nj if way == 0 else 1, rim(c)]
        dst = field.at[t + 1, 0 if way == 0 else nj + 1, rim(c)]
        where = after["rows"] if way == 0 else before["rows"]
        return remote(src, dst, z_send.at[t, way, c], z_recv.at[t, way, c], where)

    def k_copy(t, way, c):
        where = after["slabs"] if way == 0 else before["slabs"]
        return remote(
            side_out.at[t, way, :, inner(c)], side_in.at[t, way, :, inner(c)],
            k_send.at[t, way, c], k_recv.at[t, way, c], where,
        )

    def i_copy(t, way):
        src = field.at[t + 1, pl.ds(1, nj), ni if way == 0 else 1]
        dst = field.at[t + 1, pl.ds(1, nj), 0 if way == 0 else ni + 1]
        where = after["cols"] if way == 0 else before["cols"]
        return remote(src, dst, i_send.at[t, way], i_recv.at[t, way], where)

    def first_copy(way, c):
        src = p_in.at[nj - 1 if way == 0 else 0, inner(c)]
        dst = field.at[1, 0 if way == 0 else nj + 1, rim(c)]
        where = after["rows"] if way == 0 else before["rows"]
        return remote(src, dst, z_send.at[0, way, c], z_recv.at[0, way, c], where)

    def t_copy(first, size):
        lines = pl.ds(first, size)
        slot = first // small
        return remote(
            sums.at[lines], below.at[lines], t_send.at[slot], t_recv.at[slot], after["rows"]
        )

    def totals_of(q, body):
        start = piece_of(q) * width
        each(width // small, lambda n: body(start + n * small, small))

    def send_z(t, c):
        z_copy(t, 0, c).start()
        z_copy(t, 1, c).start()

    def send_sides(t, c):
        k_copy(t, 0, c).start()
        k_copy(t, 1, c).start()

        @pl.when(c == parts - 1)
        def _():
            i_copy(t, 0).start()

        @pl.when(c == 0)
        def _():
            i_copy(t, 1).start()

    def each(count, body):
        def wrapped(n, carry):
            body(n)
            return carry

        lax.fori_loop(0, count, wrapped, 0)

    for which in range(3):
        each(parts, lambda q: load(which, piece_of(q)).start())

    barrier = pltpu.get_barrier_semaphore()
    for axis in RING_AXES:
        for where in (after[axis], before[axis]):
            pl.semaphore_signal(barrier, inc=1, device_id=where, device_id_type=MESH)
    pl.semaphore_wait(barrier, 2 * len(RING_AXES))

    def begin_z(q):
        first_copy(0, piece_of(q)).start()
        first_copy(1, piece_of(q)).start()

    each(parts, begin_z)

    def begin(q):
        c = piece_of(q)
        load(0, c).wait()

        def sides(n):
            i = c * width + n
            for j in range(nj):
                side_out[0, 0, j, i] = field[1, j + 1, i + 1, nk - 1:nk]
                side_out[0, 1, j, i] = field[1, j + 1, i + 1, 0:1]

        each(width, sides)
        send_sides(0, c)

    each(parts, begin)

    def wait_loads(q):
        load(1, piece_of(q)).wait()
        load(2, piece_of(q)).wait()

    each(parts, wait_loads)

    def advance(t, q, last):
        c = piece_of(q)
        k_copy(t, 0, c).wait_recv()
        k_copy(t, 1, c).wait_recv()

        @pl.when(c == 0)
        def _():
            i_copy(t, 0).wait_recv()

        @pl.when(c == parts - 1)
        def _():
            i_copy(t, 1).wait_recv()

        z_copy(t, 0, c).wait_recv()
        z_copy(t, 1, c).wait_recv()

        def line(n):
            i = c * width + n
            level = lax.broadcasted_iota(jnp.int32, (nk, 1), 0)
            column = [field[t + 1, j, i + 1] for j in range(nj + 2)]
            run = None
            for j in range(nj):
                middle = column[j + 1]
                under = jnp.where(level == 0, side_in[t, 0, j, i], pltpu.roll(middle, 1, 0))
                over = jnp.where(
                    level == nk - 1, side_in[t, 1, j, i], pltpu.roll(middle, nk - 1, 0)
                )
                spread = (
                    column[j] + column[j + 2] + field[t + 1, j + 1, i] + field[t + 1, j + 1, i + 2]
                    + under + over - 6.0 * middle
                )
                later = 2.0 * middle - field[t, j + 1, i + 1] + speed[j, i] * spread
                if last:
                    end_out[j, i] = later
                    run = later if run is None else run + later
                    pot_out[j, i] = run
                else:
                    field[t + 2, j + 1, i + 1] = later
                    side_out[t + 1, 0, j, i] = later[nk - 1:nk]
                    side_out[t + 1, 1, j, i] = later[0:1]
            if last:
                sums[i] = run

        each(width, line)
        if last:
            @pl.when(row == 0)
            def _():
                totals_of(q, lambda first, size: t_copy(first, size).start())
        else:
            send_z(t + 1, c)
            send_sides(t + 1, c)

    each(STEPS - 1, lambda t: each(parts, lambda q: advance(t, q, False)))
    each(parts, lambda q: advance(STEPS - 1, q, True))

    def finish(q):
        c = piece_of(q)

        def one(first, size):
            t_copy(first, size).wait_recv()

            @pl.when(row < ring["rows"] - 1)
            def _():
                def passed(m):
                    sums[first + m] = sums[first + m] + below[first + m]

                each(size, passed)
                t_copy(first, size).start()

            def added(m):
                i = first + m
                base = below[i]
                for j in range(nj):
                    pot_out[j, i] = scale(pot_out[j, i] + base)

            each(size, added)

        @pl.when(row > 0)
        def _():
            totals_of(q, one)

        @pl.when(row == 0)
        def _():
            def scaled(n):
                i = c * width + n
                for j in range(nj):
                    pot_out[j, i] = scale(pot_out[j, i])

            each(width, scaled)

    each(parts, finish)

    def drain(q):
        c = piece_of(q)

        def steps(t):
            for way in range(2):
                z_copy(t, way, c).wait_send()
                k_copy(t, way, c).wait_send()

        each(STEPS, steps)

        @pl.when(row < ring["rows"] - 1)
        def _():
            totals_of(q, lambda first, size: t_copy(first, size).wait_send())

    each(parts, drain)

    def drain_ends(t):
        i_copy(t, 0).wait_send()
        i_copy(t, 1).wait_send()

    each(STEPS, drain_ends)


def local(pressure, earlier, speed_square):
    nj, ni, nk, nm = pressure.shape
    ring = {axis: lax.axis_size(axis) for axis in RING_AXES}
    parts = 2
    small = 2 if ni % (2 * parts) == 0 else 1
    cells = nj * ring["rows"]

    def scale(values):
        return values * (1.0 / cells) if cells & (cells - 1) == 0 else values / cells

    anywhere = pl.BlockSpec(memory_space=pl.ANY)
    shape = pltpu.VMEM(pressure.shape, jnp.float32)
    dma = pltpu.SemaphoreType.DMA
    return pl.pallas_call(
        functools.partial(kernel, ring, parts, small, scale),
        out_shape=(shape, shape),
        in_specs=[anywhere] * 3,
        out_specs=(pl.BlockSpec(memory_space=pltpu.VMEM),) * 2,
        scratch_shapes=[
            pltpu.VMEM((STEPS + 1, nj + 2, ni + 2, nk, nm), jnp.float32),
            pltpu.VMEM((nj, ni, nk, nm), jnp.float32),
            pltpu.VMEM((STEPS, 2, nj, ni, 1, nm), jnp.float32),
            pltpu.VMEM((STEPS, 2, nj, ni, 1, nm), jnp.float32),
            pltpu.VMEM((ni, nk, nm), jnp.float32),
            pltpu.VMEM((ni, nk, nm), jnp.float32),
            dma((3, parts)),
            dma((STEPS, 2, parts)), dma((STEPS, 2, parts)),
            dma((STEPS, 2, parts)), dma((STEPS, 2, parts)),
            dma((STEPS, 2)), dma((STEPS, 2)),
            dma((ni // small,)), dma((ni // small,)),
        ],
        compiler_params=pltpu.CompilerParams(
            collective_id=0, has_side_effects=True, vmem_limit_bytes=46 * 1024 * 1024
        ),
    )(pressure, earlier, speed_square)


def solution(mesh):
    placed = P(("site", "rows"), "cols", "slabs", None)
    return jax.shard_map(
        local, mesh=mesh, in_specs=(placed,) * 3, out_specs=(placed,) * 2, check_vma=False
    )
```
